64 devices in a mesh: dp: 4 (over x, y), sp: 16 (over z, core).
Axes of the slice: x: 2, y: 2, z: 8, core: 2. Of those that a mesh axis runs over, the one named last changes fastest.
The devices are a block of a 4x4x8 slice.
Arguments:
- resid_x: bfloat16 [32, 2048, 2048], P('dp', 'sp'), parts along dimension 0
- positions: int32 [32, 2048], P('dp', 'sp'), parts along dimension 0
- w_query: bfloat16 [2048, 2048], replicated
- w_key: bfloat16 [2048, 2048], replicated
- w_value: bfloat16 [2048, 2048], replicated
- w_out: bfloat16 [2048, 2048], replicated
- gain_q: bfloat16 [2048], replicated
- gain_k: bfloat16 [2048], replicated
- gain_out: bfloat16 [2048], replicated
Outputs:
- output: bfloat16 [32, 2048, 2048], P('dp', 'sp'), parts along dimension 0
There are 4 independent parts. The reference program is written for one: setup_inputs(seed, part) draws one part's arguments, and reference() takes and returns one part's arrays. A program takes and returns all parts, laid end to end along the dimension named above; an argument that names none is the same for every part.
All inputs are finite; a program needn't handle non-finite values.
Results may differ from the reference program's by a relative error of at most 0.0186704.
Values are sent between devices in bfloat16 or wider.
A program may use at most 768 MiB of HBM per device.

```python
import jax
import jax.numpy as jnp
from jax import lax

BATCH = 8
SEQ = 2048
D_MODEL = 2048
HEADS = 16
HEAD_DIM = 128
DOC_LEN = 512
QUERY_BLOCKS = 8
ROPE_THETA = 500000.0
NORM_EPS = 1e-6
SCALE = HEAD_DIM ** -0.5


def setup_inputs(seed: int = 0, part: int = 0) -> dict:
    base_key = jax.random.key(seed)
    shared_keys = jax.random.split(base_key, 8)
    part_keys = jax.random.split(jax.random.fold_in(shared_keys[7], part), 2)
    resid_x = jax.random.normal(part_keys[0], (BATCH, SEQ, D_MODEL), jnp.float32).astype(jnp.bfloat16)
    token_idx = jnp.arange(SEQ, dtype=jnp.int32)[None, :]
    starts = jax.random.randint(part_keys[1], (BATCH, SEQ), 0, DOC_LEN) == 0
    starts = jnp.logical_or(starts, token_idx == 0)
    last_start = lax.cummax(jnp.where(starts, token_idx, 0), axis=1)
    positions = (token_idx - last_start).astype(jnp.int32)
    w_scale = D_MODEL ** -0.5
    matrices = [(jax.random.normal(shared_keys[w_idx], (D_MODEL, D_MODEL), jnp.float32) * w_scale).astype(jnp.bfloat16) for w_idx in range(4)]
    gains = [(0.5 + jax.random.normal(shared_keys[4 + g_idx], (D_MODEL,), jnp.float32)).astype(jnp.bfloat16) for g_idx in range(3)]
    return {'resid_x': resid_x, 'positions': positions, 'w_query': matrices[0], 'w_key': matrices[1], 'w_value': matrices[2], 'w_out': matrices[3], 'gain_q': gains[0], 'gain_k': gains[1], 'gain_out': gains[2]}


def rope_tables(pos_ids):
    inv_freq = 1.0 / (ROPE_THETA ** (jnp.arange(0, HEAD_DIM, 2, dtype=jnp.float32) / HEAD_DIM))
    angles = pos_ids.astype(jnp.float32)[..., None] * inv_freq
    return jnp.cos(angles), jnp.sin(angles)


def apply_rope(heads_f32, cos_t, sin_t):
    half = HEAD_DIM // 2
    cos_b = cos_t[:, :, None, :]
    sin_b = sin_t[:, :, None, :]
    first = heads_f32[..., :half]
    second = heads_f32[..., half:]
    return jnp.concatenate([first * cos_b - second * sin_b, second * cos_b + first * sin_b], axis=-1)


def rms_scale(vals_f32, gain):
    mean_sq = jnp.mean(vals_f32 * vals_f32, axis=-1, keepdims=True)
    return vals_f32 * lax.rsqrt(mean_sq + NORM_EPS) * gain.astype(jnp.float32)


def norm_rope(x_rows, weight, gain, cos_t, sin_t):
    proj = jnp.dot(x_rows, weight, preferred_element_type=jnp.float32).astype(jnp.bfloat16).astype(jnp.float32)
    normed = rms_scale(proj, gain).reshape(BATCH, SEQ, HEADS, HEAD_DIM)
    return apply_rope(normed, cos_t, sin_t).astype(jnp.bfloat16)


def head_attention(operands):
    q_head, k_head, v_head = operands
    block = SEQ // QUERY_BLOCKS
    q_blocks = q_head.reshape(BATCH, QUERY_BLOCKS, block, HEAD_DIM).transpose(1, 0, 2, 3)
    k_f32 = k_head.astype(jnp.float32)
    v_f32 = v_head.astype(jnp.float32)
    key_idx = jnp.arange(SEQ)

    def one_block(blk_ops):
        q_blk, blk_idx = blk_ops
        scores = jnp.einsum('bqd,bkd->bqk', q_blk.astype(jnp.float32), k_f32) * SCALE
        q_idx = blk_idx * block + jnp.arange(block)
        mask = key_idx[None, :] <= q_idx[:, None]
        scores = jnp.where(mask[None], scores, -1e30)
        probs = jax.nn.softmax(scores, axis=-1).astype(jnp.bfloat16).astype(jnp.float32)
        return jnp.einsum('bqk,bkd->bqd', probs, v_f32).astype(jnp.bfloat16)

    out_blocks = lax.map(one_block, (q_blocks, jnp.arange(QUERY_BLOCKS)))
    return out_blocks.transpose(1, 0, 2, 3).reshape(BATCH, SEQ, HEAD_DIM)


def reference(resid_x, positions, w_query, w_key, w_value, w_out, gain_q, gain_k, gain_out):
    cos_t, sin_t = rope_tables(positions)
    x_rows = resid_x.reshape(BATCH * SEQ, D_MODEL)
    q_all = norm_rope(x_rows, w_query, gain_q, cos_t, sin_t)
    k_all = norm_rope(x_rows, w_key, gain_k, cos_t, sin_t)
    v_all = jnp.dot(x_rows, w_value, preferred_element_type=jnp.float32).astype(jnp.bfloat16).reshape(BATCH, SEQ, HEADS, HEAD_DIM)
    per_head = lax.map(head_attention, (q_all.transpose(2, 0, 1, 3), k_all.transpose(2, 0, 1, 3), v_all.transpose(2, 0, 1, 3)))
    attn_rows = per_head.transpose(1, 2, 0, 3).reshape(BATCH * SEQ, D_MODEL)
    attn_out = jnp.dot(attn_rows, w_out, preferred_element_type=jnp.float32).astype(jnp.bfloat16).astype(jnp.float32)
    y_rows = x_rows.astype(jnp.float32) + rms_scale(attn_out, gain_out)
    return y_rows.astype(jnp.bfloat16).reshape(BATCH, SEQ, D_MODEL)
```

```python
import functools

import jax
import jax.numpy as jnp
import numpy as np
from jax import lax
from jax.experimental import pallas as pl
from jax.experimental.pallas import tpu as pltpu
from jax.sharding import PartitionSpec as P

HEAD_DIM = 128
ROPE_THETA = 500000.0
NORM_EPS = 1e-6
SCALE = HEAD_DIM ** -0.5
LOG2E = 1.4426950408889634
MESH = pl.DeviceIdType.MESH
BF = jnp.bfloat16
F32 = jnp.float32
CORES = 2
NT = 512
HG = 4


def lane_fold(vals):
    total = vals[:, :HEAD_DIM]
    for start in range(HEAD_DIM, vals.shape[1], HEAD_DIM):
        total = total + vals[:, start:start + HEAD_DIM]
    return total


def block_kernel(n_z, x_ref, pos_ref, wq_ref, wk_ref, wv_ref, wo_ref, freq_ref, gq_ref, gk_ref, ga_ref, y_ref,
                 wbuf, xbuf, pbuf, qbuf, kbuf, vbuf, raw, obuf, sscr, acc, lsum, tabs,
                 wsem, xsend, xrecv, psend, precv, ksend, krecv, vsend, vrecv, ysend, yrecv):
    seq_loc, width = xbuf.shape[1], xbuf.shape[2]
    heads = width // HEAD_DIM
    me = lax.axis_index('sp')
    dp = lax.axis_index('dp')
    z = me // CORES
    c = me % CORES
    other = z * CORES + (1 - c)

    def peer(zz):
        return (dp, zz * CORES + c)

    def src_z(t):
        half = (t + 1) // 2
        sign = 1 - 2 * ((t + 1) % 2)
        return (z + half * sign + n_z) % n_z

    def w_copy(i, ref):
        return pltpu.make_async_copy(ref, wbuf.at[i], wsem.at[i])

    w_copies = [w_copy(0, wk_ref), w_copy(1, wv_ref), w_copy(2, wq_ref), w_copy(3, wo_ref)]

    def x_copy(zz, slot):
        return pltpu.make_async_remote_copy(src_ref=x_ref.at[zz], dst_ref=xbuf.at[slot], send_sem=xsend.at[zz],
                                            recv_sem=xrecv.at[slot], device_id=peer(zz), device_id_type=MESH)

    def p_copy(zz, slot):
        return pltpu.make_async_remote_copy(src_ref=pos_ref.at[zz], dst_ref=pbuf.at[slot], send_sem=psend.at[zz],
                                            recv_sem=precv.at[slot], device_id=peer(zz), device_id_type=MESH)

    def kv_copy(buf, ssem, rsem, zz, core):
        return pltpu.make_async_remote_copy(src_ref=buf.at[zz, core], dst_ref=buf.at[zz, core], send_sem=ssem.at[zz],
                                            recv_sem=rsem.at[zz], device_id=(dp, other), device_id_type=MESH)

    def y_copy(zz, slot):
        return pltpu.make_async_remote_copy(src_ref=xbuf.at[zz], dst_ref=y_ref.at[slot], send_sem=ysend.at[zz],
                                            recv_sem=yrecv.at[slot], device_id=peer(zz), device_id_type=MESH)

    own_x = pltpu.make_async_copy(x_ref.at[z], xbuf.at[z], xrecv.at[z])
    own_p = pltpu.make_async_copy(pos_ref.at[z], pbuf.at[z], precv.at[z])
    own_x.start()
    own_p.start()

    barrier = pltpu.get_barrier_semaphore()
    for d in range(1, n_z):
        pl.semaphore_signal(barrier, inc=1, device_id=peer((z + d) % n_z), device_id_type=MESH)
    pl.semaphore_signal(barrier, inc=1, device_id=(dp, other), device_id_type=MESH)
    pl.semaphore_wait(barrier, n_z)

    for t in range(1, n_z):
        p_copy(src_z(t), z).start()
        x_copy(src_z(t), z).start()
    for cp in w_copies:
        cp.start()

    def matmul_stats(src, wi):
        def tile(n, ss):
            cols = pl.ds(pl.multiple_of(n * NT, NT), NT)
            prod = jnp.dot(src[...], wbuf[wi, :, cols], preferred_element_type=F32).astype(BF)
            raw[:, cols] = prod
            wide = prod.astype(F32)
            return ss + lane_fold(wide * wide)
        ss = lax.fori_loop(0, width // NT, tile, jnp.zeros((seq_loc, HEAD_DIM), F32))
        return lax.rsqrt(jnp.sum(ss, axis=-1, keepdims=True) * (1.0 / width) + NORM_EPS)

    def norm_rope(scale, gain_ref, dst):
        def quad(h4, carry):
            for i in range(4):
                cols = pl.ds(pl.multiple_of((h4 * 4 + i) * HEAD_DIM, HEAD_DIM), HEAD_DIM)
                u = raw[:, cols].astype(F32) * scale * gain_ref[:, cols]
                dst[:, cols] = (u * tabs[0] + pltpu.roll(u, HEAD_DIM // 2, 1) * tabs[1]).astype(BF)
            return carry
        lax.fori_loop(0, heads // 4, quad, 0)

    def make_tables(zz):
        row = jnp.broadcast_to(pbuf[zz].astype(F32), (seq_loc, seq_loc))
        angle = jnp.transpose(row) * freq_ref[...]
        lane = lax.broadcasted_iota(jnp.int32, (seq_loc, HEAD_DIM), 1)
        sin_t = jnp.sin(angle)
        tabs[0] = jnp.cos(angle)
        tabs[1] = jnp.where(lane < HEAD_DIM // 2, -sin_t, sin_t)

    def qkv_block(zz):
        make_tables(zz)
        src = xbuf.at[zz]
        norm_rope(matmul_stats(src, 0), gk_ref, kbuf.at[zz, c])

        def v_tile(n, carry):
            cols = pl.ds(pl.multiple_of(n * NT, NT), NT)
            vbuf[zz, c, :, cols] = jnp.dot(src[...], wbuf[1, :, cols], preferred_element_type=F32).astype(BF)
            return carry
        lax.fori_loop(0, width // NT, v_tile, 0)
        kv_copy(kbuf, ksend, krecv, zz, c).start()
        norm_rope(matmul_stats(src, 2), gq_ref, qbuf.at[zz])
        kv_copy(vbuf, vsend, vrecv, zz, c).start()

    own_x.wait()
    own_p.wait()
    for cp in w_copies[:3]:
        cp.wait()
    qkv_block(z)

    def phase1(t, carry):
        zz = src_z(t)
        p_copy(z, zz).wait_recv()
        x_copy(z, zz).wait_recv()
        qkv_block(zz)
        return carry
    lax.fori_loop(1, n_z, phase1, 0)

    w_copies[3].wait()

    def kv_wait(zz, carry):
        kv_copy(kbuf, ksend, krecv, zz, 1 - c).wait_recv()
        kv_copy(vbuf, vsend, vrecv, zz, 1 - c).wait_recv()
        return carry
    lax.fori_loop(0, n_z, kv_wait, 0)

    keys = CORES * seq_loc
    lim = SCALE * LOG2E

    def attend(zz):
        def group(g, carry):
            def cols_of(i):
                return pl.ds(pl.multiple_of((g * HG + i) * HEAD_DIM, HEAD_DIM), HEAD_DIM)

            def score(i, kz):
                k = kbuf[kz, :, :, cols_of(i)].reshape(keys, HEAD_DIM)
                return lax.dot_general(qbuf[zz, :, cols_of(i)], k, (((1,), (1,)), ((), ())), preferred_element_type=F32)

            row = lax.broadcasted_iota(jnp.int32, (seq_loc, keys), 0) + c * seq_loc
            col = lax.broadcasted_iota(jnp.int32, (seq_loc, keys), 1)
            tops = []
            for i in range(HG):
                s = jnp.where(col <= row, score(i, zz), -1e30)
                sscr[i, zz] = s
                tops.append(jnp.maximum(s[:, :seq_loc], s[:, seq_loc:]))

            def body_a(kz, tops):
                new = []
                for i in range(HG):
                    s = score(i, kz)
                    sscr[i, kz] = s
                    new.append(jnp.maximum(tops[i], jnp.maximum(s[:, :seq_loc], s[:, seq_loc:])))
                return tuple(new)
            tops = lax.fori_loop(0, zz, body_a, tuple(tops))
            peak = [jnp.max(t, axis=-1, keepdims=True) for t in tops]
            for i in range(HG):
                acc[i] = jnp.zeros((seq_loc, HEAD_DIM), F32)
                lsum[i] = jnp.zeros((seq_loc, HEAD_DIM), F32)

            def body_b(kz, carry):
                for i in range(HG):
                    p = jnp.exp2((sscr[i, kz] - peak[i]) * lim)
                    lsum[i] += p[:, :seq_loc] + p[:, seq_loc:]
                    v = vbuf[kz, :, :, cols_of(i)].reshape(keys, HEAD_DIM)
                    acc[i] += jnp.dot(p.astype(BF), v, preferred_element_type=F32)
                return carry
            lax.fori_loop(0, zz + 1, body_b, 0)
            for i in range(HG):
                total = jnp.sum(lsum[i], axis=-1, keepdims=True)
                obuf[:, cols_of(i)] = (acc[i] / total).astype(BF)
            return carry
        lax.fori_loop(0, heads // HG, group, 0)

    def out_block(zz):
        scale = matmul_stats(obuf, 3)

        def tile(n, carry):
            cols = pl.ds(pl.multiple_of(n * NT, NT), NT)
            y = xbuf[zz, :, cols].astype(F32) + raw[:, cols].astype(F32) * scale * ga_ref[:, cols]
            xbuf[zz, :, cols] = y.astype(BF)
            return carry
        lax.fori_loop(0, width // NT, tile, 0)

    def phase2(u, carry):
        zz = src_z(n_z - 1 - u)
        attend(zz)
        out_block(zz)
        y_copy(zz, z).start()
        return carry
    lax.fori_loop(0, n_z - 1, phase2, 0)
    attend(z)
    out_block(z)
    own_y = pltpu.make_async_copy(xbuf.at[z], y_ref.at[z], yrecv.at[z])
    own_y.start()

    def drain(t, carry):
        zz = src_z(t)
        p_copy(zz, z).wait_send()
        x_copy(zz, z).wait_send()
        y_copy(zz, z).wait_send()
        y_copy(z, zz).wait_recv()
        return carry
    lax.fori_loop(1, n_z, drain, 0)

    def kv_drain(zz, carry):
        kv_copy(kbuf, ksend, krecv, zz, c).wait_send()
        kv_copy(vbuf, vsend, vrecv, zz, c).wait_send()
        return carry
    lax.fori_loop(0, n_z, kv_drain, 0)
    own_y.wait()


def solution(mesh):
    n_z = mesh.shape['sp'] // CORES

    def local_block(x_loc, pos_loc, w_query, w_key, w_value, w_out, gain_q, gain_k, gain_out):
        batch, seq_loc, width = x_loc.shape
        inv_freq = 1.0 / (ROPE_THETA ** (np.arange(0, HEAD_DIM, 2, dtype=np.float32) / HEAD_DIM))
        freq = jnp.asarray(np.concatenate([inv_freq, inv_freq]).astype(np.float32)[None, :])
        any_spec = pl.BlockSpec(memory_space=pl.ANY)
        vmem = pl.BlockSpec(memory_space=pltpu.VMEM)
        dma = pltpu.SemaphoreType.DMA
        f32_gain = [g.astype(F32)[None, :] for g in (gain_q, gain_k, gain_out)]
        return pl.pallas_call(
            functools.partial(block_kernel, n_z),
            out_shape=jax.ShapeDtypeStruct(x_loc.shape, BF),
            in_specs=[any_spec] * 6 + [vmem] * 4,
            out_specs=any_spec,
            scratch_shapes=[
                pltpu.VMEM((4, width, width), BF),
                pltpu.VMEM((n_z, seq_loc, width), BF),
                pltpu.VMEM((n_z, 1, seq_loc), jnp.int32),
                pltpu.VMEM((n_z, seq_loc, width), BF),
                pltpu.VMEM((n_z, CORES, seq_loc, width), BF),
                pltpu.VMEM((n_z, CORES, seq_loc, width), BF),
                pltpu.VMEM((seq_loc, width), BF),
                pltpu.VMEM((seq_loc, width), BF),
                pltpu.VMEM((HG, n_z, seq_loc, CORES * seq_loc), F32),
                pltpu.VMEM((HG, seq_loc, HEAD_DIM), F32),
                pltpu.VMEM((HG, seq_loc, HEAD_DIM), F32),
                pltpu.VMEM((2, seq_loc, HEAD_DIM), F32),
                dma((4,)),
            ] + [dma((n_z,))] * 10,
            compiler_params=pltpu.CompilerParams(collective_id=0, has_side_effects=True, vmem_limit_bytes=67043328),
        )(x_loc, pos_loc[:, None, :], w_query, w_key, w_value, w_out, freq, *f32_gain)

    tok_spec = P('dp', 'sp', None)
    return jax.shard_map(local_block, mesh=mesh, in_specs=(tok_spec, P('dp', 'sp'), P(), P(), P(), P(), P(), P(), P()), out_specs=tok_spec, check_vma=False)
```

```python
import functools

import jax
import jax.numpy as jnp
import numpy as np
from jax import lax
from jax.experimental import pallas as pl
from jax.experimental.pallas import tpu as pltpu
from jax.sharding import PartitionSpec as P

HEAD_DIM = 128
ROPE_THETA = 500000.0
NORM_EPS = 1e-6
SCALE = HEAD_DIM ** -0.5
LOG2E = 1.4426950408889634
MESH = pl.DeviceIdType.MESH
BF = jnp.bfloat16
F32 = jnp.float32
CORES = 2
NT = 1024
RG = 8
MAX_HG = 4
SLOTS = 16


def lane_fold(vals):
    total = vals[:, :HEAD_DIM]
    for start in range(HEAD_DIM, vals.shape[1], HEAD_DIM):
        total = total + vals[:, start:start + HEAD_DIM]
    return total


def block_kernel(n_z, x_ref, pos_ref, wq_ref, wk_ref, wv_ref, wo_ref, freq_ref, gq_ref, gk_ref, ga_ref, y_ref,
                 wbuf, xbuf, pbuf, qbuf, kbuf, vbuf, raw, sscr, gains, tabs,
                 wsem, xsend, xrecv, psend, precv, ksend, krecv, vsend, vrecv, ysend, yrecv):
    seq_loc, width = xbuf.shape[1], xbuf.shape[2]
    heads = width // HEAD_DIM
    me = lax.axis_index('sp')
    dp = lax.axis_index('dp')
    z = me // CORES
    c = me % CORES
    other = z * CORES + (1 - c)

    def peer(zz):
        return (dp, zz * CORES + c)

    def src_z(t):
        half = (t + 1) // 2
        sign = 1 - 2 * ((t + 1) % 2)
        return (z + half * sign + n_z) % n_z

    def w_copy(i, ref):
        return pltpu.make_async_copy(ref, wbuf.at[i], wsem.at[i])

    w_copies = [w_copy(0, wk_ref), w_copy(1, wv_ref), w_copy(2, wq_ref), w_copy(3, wo_ref)]

    def x_copy(zz, slot):
        return pltpu.make_async_remote_copy(src_ref=x_ref.at[zz], dst_ref=xbuf.at[slot], send_sem=xsend.at[zz],
                                            recv_sem=xrecv.at[slot], device_id=peer(zz), device_id_type=MESH)

    def p_copy(zz, slot):
        return pltpu.make_async_remote_copy(src_ref=pos_ref.at[zz], dst_ref=pbuf.at[slot], send_sem=psend.at[zz],
                                            recv_sem=precv.at[slot], device_id=peer(zz), device_id_type=MESH)

    def kv_copy(buf, ssem, rsem, zz, core):
        return pltpu.make_async_remote_copy(src_ref=buf.at[zz, core], dst_ref=buf.at[zz, core], send_sem=ssem.at[zz],
                                            recv_sem=rsem.at[zz], device_id=(dp, other), device_id_type=MESH)

    def y_copy(zz, slot):
        return pltpu.make_async_remote_copy(src_ref=xbuf.at[zz], dst_ref=y_ref.at[slot], send_sem=ysend.at[zz],
                                            recv_sem=yrecv.at[slot], device_id=peer(zz), device_id_type=MESH)

    own_x = pltpu.make_async_copy(x_ref.at[z], xbuf.at[z], xrecv.at[z])
    own_p = pltpu.make_async_copy(pos_ref.at[z], pbuf.at[z], precv.at[z])
    own_x.start()
    own_p.start()
    for cp in w_copies:
        cp.start()

    for i, ref in enumerate((gq_ref, gk_ref, ga_ref)):
        for h in range(heads):
            gains[i, h] = ref[h * HEAD_DIM:(h + 1) * HEAD_DIM].astype(F32)[None, :]

    barrier = pltpu.get_barrier_semaphore()
    for d in range(1, n_z):
        pl.semaphore_signal(barrier, inc=1, device_id=peer((z + d) % n_z), device_id_type=MESH)
    pl.semaphore_signal(barrier, inc=1, device_id=(dp, other), device_id_type=MESH)
    pl.semaphore_wait(barrier, n_z)

    for t in range(1, n_z):
        p_copy(src_z(t), z).start()
        x_copy(src_z(t), z).start()

    def matmul_stats(load, wi):
        per = NT // HEAD_DIM

        def tile(n, ss):
            cols = pl.ds(pl.multiple_of(n * NT, NT), NT)
            prod = jnp.dot(load(), wbuf[wi, :, cols], preferred_element_type=F32).astype(BF)
            for i in range(per):
                part = prod[:, i * HEAD_DIM:(i + 1) * HEAD_DIM]
                raw[n * per + i] = part
                wide = part.astype(F32)
                ss = ss + wide * wide
            return ss
        ss = lax.fori_loop(0, width // NT, tile, jnp.zeros((seq_loc, HEAD_DIM), F32))
        return lax.rsqrt(jnp.sum(ss, axis=-1, keepdims=True) * (1.0 / width) + NORM_EPS)

    def norm_rope(scale, gain_ref, dst):
        def some(hg, carry):
            for i in range(RG):
                h = hg * RG + i
                u = raw[h].astype(F32) * scale * gain_ref[h]
                dst[h] = (u * tabs[0] + pltpu.roll(u, HEAD_DIM // 2, 1) * tabs[1]).astype(BF)
            return carry
        lax.fori_loop(0, heads // RG, some, 0)

    def make_tables(zz):
        row = jnp.broadcast_to(pbuf[zz].astype(F32), (seq_loc, seq_loc))
        angle = jnp.transpose(row) * freq_ref[...]
        lane = lax.broadcasted_iota(jnp.int32, (seq_loc, HEAD_DIM), 1)
        sin_t = jnp.sin(angle)
        tabs[0] = jnp.cos(angle)
        tabs[1] = jnp.where(lane < HEAD_DIM // 2, -sin_t, sin_t)

    def qkv_block(zz):
        make_tables(zz)
        src = xbuf.at[zz]
        norm_rope(matmul_stats(lambda: src[...], 0), gains.at[1], kbuf.at[zz, c])

        def v_tile(n, carry):
            cols = pl.ds(pl.multiple_of(n * NT, NT), NT)
            prod = jnp.dot(src[...], wbuf[1, :, cols], preferred_element_type=F32).astype(BF)
            for i in range(NT // HEAD_DIM):
                vbuf[zz, c, n * (NT // HEAD_DIM) + i] = prod[:, i * HEAD_DIM:(i + 1) * HEAD_DIM]
            return carry
        lax.fori_loop(0, width // NT, v_tile, 0)
        kv_copy(kbuf, ksend, krecv, zz, c).start()
        norm_rope(matmul_stats(lambda: src[...], 2), gains.at[0], qbuf.at[zz])
        kv_copy(vbuf, vsend, vrecv, zz, c).start()

    own_x.wait()
    own_p.wait()
    for cp in w_copies[:3]:
        cp.wait()

    def phase1(t, carry):
        zz = src_z(t)

        @pl.when(t > 0)
        def _():
            p_copy(z, zz).wait_recv()
            x_copy(z, zz).wait_recv()
        qkv_block(zz)
        return carry
    lax.fori_loop(0, n_z, phase1, 0)

    w_copies[3].wait()

    def kv_wait(zz, carry):
        kv_copy(kbuf, ksend, krecv, zz, 1 - c).wait_recv()
        kv_copy(vbuf, vsend, vrecv, zz, 1 - c).wait_recv()
        return carry
    lax.fori_loop(0, n_z, kv_wait, 0)

    keys = CORES * seq_loc
    lim = SCALE * LOG2E

    def attend_len(zz, nk):
        hg = MAX_HG if nk * MAX_HG <= SLOTS else 2
        row = lax.broadcasted_iota(jnp.int32, (seq_loc, keys), 0) + c * seq_loc
        col = lax.broadcasted_iota(jnp.int32, (seq_loc, keys), 1)
        seen = col <= row

        def group(g, carry):
            peak = []
            for i in range(hg):
                h = g * hg + i
                q = qbuf[zz, h]
                top = None
                for kz in range(nk):
                    k = kbuf[kz, :, h].reshape(keys, HEAD_DIM)
                    s = lax.dot_general(q, k, (((1,), (1,)), ((), ())), preferred_element_type=F32)
                    if kz == nk - 1:
                        s = jnp.where(seen, s, -1e30)
                    sscr[i * nk + kz] = s
                    fold = jnp.maximum(s[:, :seq_loc], s[:, seq_loc:])
                    top = fold if top is None else jnp.maximum(top, fold)
                peak.append(jnp.max(top, axis=-1, keepdims=True))
            for i in range(hg):
                h = g * hg + i
                total = None
                probs = []
                for kz in range(nk):
                    p = jnp.exp2((sscr[i * nk + kz] - peak[i]) * lim)
                    fold = p[:, :seq_loc] + p[:, seq_loc:]
                    total = fold if total is None else total + fold
                    probs.append(p.astype(BF))
                v = jnp.concatenate([vbuf[kz, :, h].reshape(keys, HEAD_DIM) for kz in range(nk)], axis=0)
                out = jnp.dot(jnp.concatenate(probs, axis=1), v, preferred_element_type=F32)
                denom = jnp.sum(total, axis=-1, keepdims=True)
                qbuf[zz, h] = (out / denom).astype(BF)
            return carry
        lax.fori_loop(0, heads // hg, group, 0)

    def attend(zz):
        for nk in range(1, n_z + 1):
            pl.when(zz == nk - 1)(functools.partial(attend_len, zz, nk))

    def out_block(zz):
        scale = matmul_stats(lambda: jnp.concatenate([qbuf[zz, h] for h in range(heads)], axis=1), 3)

        def some(hg, carry):
            for i in range(RG):
                h = hg * RG + i
                cols = pl.ds(pl.multiple_of(h * HEAD_DIM, HEAD_DIM), HEAD_DIM)
                y = xbuf[zz, :, cols].astype(F32) + raw[h].astype(F32) * scale * gains[2, h]
                xbuf[zz, :, cols] = y.astype(BF)
            return carry
        lax.fori_loop(0, heads // RG, some, 0)

    own_y = pltpu.make_async_copy(xbuf.at[z], y_ref.at[z], yrecv.at[z])

    def phase2(u, carry):
        zz = src_z(n_z - 1 - u)
        attend(zz)
        out_block(zz)

        @pl.when(u < n_z - 1)
        def _():
            y_copy(zz, z).start()
        return carry
    lax.fori_loop(0, n_z, phase2, 0)
    own_y.start()

    def drain(t, carry):
        zz = src_z(t)
        p_copy(zz, z).wait_send()
        x_copy(zz, z).wait_send()
        y_copy(zz, z).wait_send()
        y_copy(z, zz).wait_recv()
        return carry
    lax.fori_loop(1, n_z, drain, 0)

    def kv_drain(zz, carry):
        kv_copy(kbuf, ksend, krecv, zz, c).wait_send()
        kv_copy(vbuf, vsend, vrecv, zz, c).wait_send()
        return carry
    lax.fori_loop(0, n_z, kv_drain, 0)
    own_y.wait()


def solution(mesh):
    n_z = mesh.shape['sp'] // CORES

    def local_block(x_loc, pos_loc, w_query, w_key, w_value, w_out, gain_q, gain_k, gain_out):
        batch, seq_loc, width = x_loc.shape
        inv_freq = 1.0 / (ROPE_THETA ** (np.arange(0, HEAD_DIM, 2, dtype=np.float32) / HEAD_DIM))
        freq = jnp.asarray(np.concatenate([inv_freq, inv_freq]).astype(np.float32)[None, :])
        heads = width // HEAD_DIM
        any_spec = pl.BlockSpec(memory_space=pl.ANY)
        vmem = pl.BlockSpec(memory_space=pltpu.VMEM)
        dma = pltpu.SemaphoreType.DMA
        return pl.pallas_call(
            functools.partial(block_kernel, n_z),
            out_shape=jax.ShapeDtypeStruct(x_loc.shape, BF),
            in_specs=[any_spec] * 6 + [vmem] * 4,
            out_specs=any_spec,
            scratch_shapes=[
                pltpu.VMEM((4, width, width), BF),
                pltpu.VMEM((n_z, seq_loc, width), BF),
                pltpu.VMEM((n_z, 1, seq_loc), jnp.int32),
                pltpu.VMEM((n_z, heads, seq_loc, HEAD_DIM), BF),
                pltpu.VMEM((n_z, CORES, heads, seq_loc, HEAD_DIM), BF),
                pltpu.VMEM((n_z, CORES, heads, seq_loc, HEAD_DIM), BF),
                pltpu.VMEM((heads, seq_loc, HEAD_DIM), BF),
                pltpu.VMEM((SLOTS, seq_loc, CORES * seq_loc), F32),
                pltpu.VMEM((3, heads, 1, HEAD_DIM), F32),
                pltpu.VMEM((2, seq_loc, HEAD_DIM), F32),
                dma((4,)),
            ] + [dma((n_z,))] * 10,
            compiler_params=pltpu.CompilerParams(collective_id=0, has_side_effects=True, vmem_limit_bytes=67043328),
        )(x_loc, pos_loc[:, None, :], w_query, w_key, w_value, w_out, freq, gain_q, gain_k, gain_out)

    tok_spec = P('dp', 'sp', None)
    return jax.shard_map(local_block, mesh=mesh, in_specs=(tok_spec, P('dp', 'sp'), P(), P(), P(), P(), P(), P(), P()), out_specs=tok_spec, check_vma=False)
```

```python
import functools

import jax
import jax.numpy as jnp
import numpy as np
from jax import lax
from jax.experimental import pallas as pl
from jax.experimental.pallas import tpu as pltpu
from jax.sharding import PartitionSpec as P

HEAD_DIM = 128
ROPE_THETA = 500000.0
NORM_EPS = 1e-6
SCALE = HEAD_DIM ** -0.5
LOG2E = 1.4426950408889634
MESH = pl.DeviceIdType.MESH
BF = jnp.bfloat16
F32 = jnp.float32
CORES = 2
NT = 1024
RG = 8
MAX_HG = 4
SLOTS = 16
PER_WORD = 6
SENDS = [
    [1, 7, 2, 6, 3, 5, 4],
    [1, 7, 2, 6, 3, 5, 4],
    [1, 7, 2, 6, 3, 5, 4],
    [1, 7, 2, 6, 3, 5, 4],
    [1, 7, 2, 6, 3, 5, 4],
    [1, 7, 2, 6, 3, 5, 4],
    [1, 7, 2, 6, 3, 5, 4],
    [1, 7, 2, 6, 3, 5, 4],
]
STEPS = [
    [0, 1, 6, 3, 2, 5, 10, 4, 12, 13, 7, 11, 9, 14, 8, 15],
    [0, 7, 6, 2, 8, 5, 3, 1, 4, 12, 10, 9, 14, 13, 11, 15],
    [0, 7, 2, 1, 6, 5, 9, 3, 4, 12, 8, 11, 14, 13, 10, 15],
    [0, 1, 7, 2, 6, 5, 13, 3, 11, 4, 12, 9, 14, 8, 15, 10],
    [0, 5, 4, 12, 2, 7, 1, 6, 8, 9, 15, 3, 10, 13, 14, 11],
    [0, 3, 2, 11, 1, 4, 12, 5, 7, 13, 6, 9, 15, 10, 14, 8],
    [0, 6, 3, 1, 2, 11, 4, 12, 5, 7, 13, 9, 8, 10, 15, 14],
    [0, 2, 7, 3, 1, 5, 4, 12, 11, 6, 15, 9, 10, 14, 8, 13],
]


def lane_fold(vals):
    total = vals[:, :HEAD_DIM]
    for start in range(HEAD_DIM, vals.shape[1], HEAD_DIM):
        total = total + vals[:, start:start + HEAD_DIM]
    return total


def block_kernel(n_z, x_ref, pos_ref, wq_ref, wk_ref, wv_ref, wo_ref, freq_ref, gq_ref, gk_ref, ga_ref, y_ref,
                 wbuf, xbuf, pbuf, qbuf, kbuf, vbuf, raw, sscr, gains, tabs,
                 wsem, xsend, xrecv, psend, precv, ksend, krecv, vsend, vrecv, ysend, yrecv):
    seq_loc, width = xbuf.shape[1], xbuf.shape[2]
    heads = width // HEAD_DIM
    me = lax.axis_index('sp')
    dp = lax.axis_index('dp')
    z = me // CORES
    c = me % CORES
    other = z * CORES + (1 - c)

    def peer(zz):
        return (dp, zz * CORES + c)

    def code_at(rows, i):
        val = jnp.int32(0)
        for start in range(0, len(rows[0]), PER_WORD):
            words = [sum(v << (4 * j) for j, v in enumerate(row[start:start + PER_WORD])) for row in rows]
            word = jnp.int32(words[0])
            for q, w in enumerate(words[1:], 1):
                word = jnp.where(z == q, w, word)
            val = jnp.where(i >= start, word, val)
        return lax.shift_right_logical(val, jnp.int32(4 * (i % PER_WORD))) % 16

    def w_copy(i, ref):
        return pltpu.make_async_copy(ref, wbuf.at[i], wsem.at[i])

    w_copies = [w_copy(0, wk_ref), w_copy(1, wv_ref), w_copy(2, wq_ref), w_copy(3, wo_ref)]

    def x_copy(zz, slot):
        return pltpu.make_async_remote_copy(src_ref=x_ref.at[zz], dst_ref=xbuf.at[slot], send_sem=xsend.at[zz],
                                            recv_sem=xrecv.at[slot], device_id=peer(zz), device_id_type=MESH)

    def p_copy(zz, slot):
        return pltpu.make_async_remote_copy(src_ref=pos_ref.at[zz], dst_ref=pbuf.at[slot], send_sem=psend.at[zz],
                                            recv_sem=precv.at[slot], device_id=peer(zz), device_id_type=MESH)

    def kv_copy(buf, ssem, rsem, zz, core):
        return pltpu.make_async_remote_copy(src_ref=buf.at[zz, core], dst_ref=buf.at[zz, core], send_sem=ssem.at[zz],
                                            recv_sem=rsem.at[zz], device_id=(dp, other), device_id_type=MESH)

    def y_copy(zz, slot):
        return pltpu.make_async_remote_copy(src_ref=xbuf.at[zz], dst_ref=y_ref.at[slot], send_sem=ysend.at[zz],
                                            recv_sem=yrecv.at[slot], device_id=peer(zz), device_id_type=MESH)

    own_x = pltpu.make_async_copy(x_ref.at[z], xbuf.at[z], xrecv.at[z])
    own_p = pltpu.make_async_copy(pos_ref.at[z], pbuf.at[z], precv.at[z])
    own_x.start()
    own_p.start()
    for cp in w_copies:
        cp.start()

    for i, ref in enumerate((gq_ref, gk_ref, ga_ref)):
        for h in range(heads):
            gains[i, h] = ref[h * HEAD_DIM:(h + 1) * HEAD_DIM].astype(F32)[None, :]

    barrier = pltpu.get_barrier_semaphore()
    for d in range(1, n_z):
        pl.semaphore_signal(barrier, inc=1, device_id=peer((z + d) % n_z), device_id_type=MESH)
    pl.semaphore_signal(barrier, inc=1, device_id=(dp, other), device_id_type=MESH)
    pl.semaphore_wait(barrier, n_z)

    for i in range(n_z - 1):
        zz = (z + code_at(SENDS, i)) % n_z
        p_copy(zz, z).start()
        x_copy(zz, z).start()

    def matmul_stats(load, wi):
        per = NT // HEAD_DIM

        def tile(n, ss):
            cols = pl.ds(pl.multiple_of(n * NT, NT), NT)
            prod = jnp.dot(load(), wbuf[wi, :, cols], preferred_element_type=F32).astype(BF)
            for i in range(per):
                part = prod[:, i * HEAD_DIM:(i + 1) * HEAD_DIM]
                raw[n * per + i] = part
                wide = part.astype(F32)
                ss = ss + wide * wide
            return ss
        ss = lax.fori_loop(0, width // NT, tile, jnp.zeros((seq_loc, HEAD_DIM), F32))
        return lax.rsqrt(jnp.sum(ss, axis=-1, keepdims=True) * (1.0 / width) + NORM_EPS)

    def norm_rope(scale, gain_ref, dst):
        def some(hg, carry):
            for i in range(RG):
                h = hg * RG + i
                u = raw[h].astype(F32) * scale * gain_ref[h]
                dst[h] = (u * tabs[0] + pltpu.roll(u, HEAD_DIM // 2, 1) * tabs[1]).astype(BF)
            return carry
        lax.fori_loop(0, heads // RG, some, 0)

    def make_tables(zz):
        row = jnp.broadcast_to(pbuf[zz].astype(F32), (seq_loc, seq_loc))
        angle = jnp.transpose(row) * freq_ref[...]
        lane = lax.broadcasted_iota(jnp.int32, (seq_loc, HEAD_DIM), 1)
        sin_t = jnp.sin(angle)
        tabs[0] = jnp.cos(angle)
        tabs[1] = jnp.where(lane < HEAD_DIM // 2, -sin_t, sin_t)

    def qkv_block(zz):
        make_tables(zz)
        src = xbuf.at[zz]
        norm_rope(matmul_stats(lambda: src[...], 0), gains.at[1], kbuf.at[zz, c])

        def v_tile(n, carry):
            cols = pl.ds(pl.multiple_of(n * NT, NT), NT)
            prod = jnp.dot(src[...], wbuf[1, :, cols], preferred_element_type=F32).astype(BF)
            for i in range(NT // HEAD_DIM):
                vbuf[zz, c, n * (NT // HEAD_DIM) + i] = prod[:, i * HEAD_DIM:(i + 1) * HEAD_DIM]
            return carry
        lax.fori_loop(0, width // NT, v_tile, 0)
        kv_copy(kbuf, ksend, krecv, zz, c).start()
        q_scale = matmul_stats(lambda: src[...], 2)
        kv_copy(vbuf, vsend, vrecv, zz, c).start()
        norm_rope(q_scale, gains.at[0], qbuf.at[zz])

    own_x.wait()
    own_p.wait()
    for cp in w_copies:
        cp.wait()


    keys = CORES * seq_loc
    lim = SCALE * LOG2E

    def attend_len(zz, nk):
        hg = MAX_HG if nk * MAX_HG <= SLOTS else 2
        row = lax.broadcasted_iota(jnp.int32, (seq_loc, keys), 0) + c * seq_loc
        col = lax.broadcasted_iota(jnp.int32, (seq_loc, keys), 1)
        seen = col <= row

        def group(g, carry):
            peak = []
            for i in range(hg):
                h = g * hg + i
                q = qbuf[zz, h]
                top = None
                for kz in range(nk):
                    k = kbuf[kz, :, h].reshape(keys, HEAD_DIM)
                    s = lax.dot_general(q, k, (((1,), (1,)), ((), ())), preferred_element_type=F32)
                    if kz == nk - 1:
                        s = jnp.where(seen, s, -1e30)
                    sscr[i * nk + kz] = s
                    fold = jnp.maximum(s[:, :seq_loc], s[:, seq_loc:])
                    top = fold if top is None else jnp.maximum(top, fold)
                peak.append(jnp.max(top, axis=-1, keepdims=True))
            for i in range(hg):
                h = g * hg + i
                total = None
                probs = []
                for kz in range(nk):
                    p = jnp.exp2((sscr[i * nk + kz] - peak[i]) * lim)
                    fold = p[:, :seq_loc] + p[:, seq_loc:]
                    total = fold if total is None else total + fold
                    probs.append(p.astype(BF))
                v = jnp.concatenate([vbuf[kz, :, h].reshape(keys, HEAD_DIM) for kz in range(nk)], axis=0)
                out = jnp.dot(jnp.concatenate(probs, axis=1), v, preferred_element_type=F32)
                denom = jnp.sum(total, axis=-1, keepdims=True)
                qbuf[zz, h] = (out / denom).astype(BF)
            return carry
        lax.fori_loop(0, heads // hg, group, 0)

    def attend(zz):
        for nk in range(1, n_z + 1):
            pl.when(zz == nk - 1)(functools.partial(attend_len, zz, nk))

    def out_block(zz):
        scale = matmul_stats(lambda: jnp.concatenate([qbuf[zz, h] for h in range(heads)], axis=1), 3)

        def some(hg, carry):
            for i in range(RG):
                h = hg * RG + i
                cols = pl.ds(pl.multiple_of(h * HEAD_DIM, HEAD_DIM), HEAD_DIM)
                y = xbuf[zz, :, cols].astype(F32) + raw[h].astype(F32) * scale * gains[2, h]
                xbuf[zz, :, cols] = y.astype(BF)
            return carry
        lax.fori_loop(0, heads // RG, some, 0)

    own_y = pltpu.make_async_copy(xbuf.at[z], y_ref.at[z], yrecv.at[z])

    def step(i, done):
        code = code_at(STEPS, i)
        zz = (z + code) % n_z

        @pl.when(code < n_z)
        def _():
            @pl.when(code > 0)
            def _():
                p_copy(z, zz).wait_recv()
                x_copy(z, zz).wait_recv()
            qkv_block(zz)

        @pl.when(code >= n_z)
        def _():
            def kv_wait(j, carry):
                prev = code_at(STEPS, j)

                @pl.when(prev < n_z)
                def _():
                    src = (z + prev) % n_z
                    kv_copy(kbuf, ksend, krecv, src, 1 - c).wait_recv()
                    kv_copy(vbuf, vsend, vrecv, src, 1 - c).wait_recv()
                return carry
            lax.fori_loop(done, i, kv_wait, 0)
            attend(zz)
            out_block(zz)

            @pl.when(code > n_z)
            def _():
                y_copy(zz, z).start()

            @pl.when(code == n_z)
            def _():
                own_y.start()
        return jnp.where(code < n_z, done, i)
    lax.fori_loop(0, 2 * n_z, step, 0)

    def drain(t, carry):
        zz = (z + t) % n_z
        p_copy(zz, z).wait_send()
        x_copy(zz, z).wait_send()
        y_copy(zz, z).wait_send()
        y_copy(z, zz).wait_recv()
        return carry
    lax.fori_loop(1, n_z, drain, 0)

    def kv_drain(zz, carry):
        kv_copy(kbuf, ksend, krecv, zz, c).wait_send()
        kv_copy(vbuf, vsend, vrecv, zz, c).wait_send()
        return carry
    lax.fori_loop(0, n_z, kv_drain, 0)
    own_y.wait()


def copy_kernel(src_ref, dst_ref, buf, in_sem, out_sem):
    parts = src_ref.shape[0]
    reads = [pltpu.make_async_copy(src_ref.at[i], buf.at[i], in_sem.at[i]) for i in range(parts)]
    writes = [pltpu.make_async_copy(buf.at[i], dst_ref.at[i], out_sem.at[i]) for i in range(parts)]
    for cp in reads:
        cp.start()
    for rd, wr in zip(reads, writes):
        rd.wait()
        wr.start()
    for cp in writes:
        cp.wait()


def solution(mesh):
    n_z = mesh.shape['sp'] // CORES

    def local_block(x_loc, pos_loc, w_query, w_key, w_value, w_out, gain_q, gain_k, gain_out):
        batch, seq_loc, width = x_loc.shape
        inv_freq = 1.0 / (ROPE_THETA ** (np.arange(0, HEAD_DIM, 2, dtype=np.float32) / HEAD_DIM))
        freq = jnp.asarray(np.concatenate([inv_freq, inv_freq]).astype(np.float32)[None, :])
        heads = width // HEAD_DIM
        any_spec = pl.BlockSpec(memory_space=pl.ANY)
        vmem = pl.BlockSpec(memory_space=pltpu.VMEM)
        dma = pltpu.SemaphoreType.DMA
        y_home = pl.pallas_call(
            functools.partial(block_kernel, n_z),
            out_shape=jax.ShapeDtypeStruct(x_loc.shape, BF),
            in_specs=[any_spec] * 6 + [vmem] * 4,
            out_specs=any_spec,
            scratch_shapes=[
                pltpu.VMEM((4, width, width), BF),
                pltpu.VMEM((n_z, seq_loc, width), BF),
                pltpu.VMEM((n_z, 1, seq_loc), jnp.int32),
                pltpu.VMEM((n_z, heads, seq_loc, HEAD_DIM), BF),
                pltpu.VMEM((n_z, CORES, heads, seq_loc, HEAD_DIM), BF),
                pltpu.VMEM((n_z, CORES, heads, seq_loc, HEAD_DIM), BF),
                pltpu.VMEM((heads, seq_loc, HEAD_DIM), BF),
                pltpu.VMEM((SLOTS, seq_loc, CORES * seq_loc), F32),
                pltpu.VMEM((3, heads, 1, HEAD_DIM), F32),
                pltpu.VMEM((2, seq_loc, HEAD_DIM), F32),
                dma((4,)),
            ] + [dma((n_z,))] * 10,
            compiler_params=pltpu.CompilerParams(collective_id=0, has_side_effects=True, vmem_limit_bytes=67043328),
        )(x_loc, pos_loc[:, None, :], w_query, w_key, w_value, w_out, freq, gain_q, gain_k, gain_out)
        return pl.pallas_call(
            copy_kernel,
            out_shape=jax.ShapeDtypeStruct(x_loc.shape, BF),
            in_specs=[any_spec],
            out_specs=any_spec,
            scratch_shapes=[pltpu.VMEM(x_loc.shape, BF), dma((batch,)), dma((batch,))],
        )(y_home)

    tok_spec = P('dp', 'sp', None)
    return jax.shard_map(local_block, mesh=mesh, in_specs=(tok_spec, P('dp', 'sp'), P(), P(), P(), P(), P(), P(), P()), out_specs=tok_spec, check_vma=False)
```

```python
import functools

import jax
import jax.numpy as jnp
import numpy as np
from jax import lax
from jax.experimental import pallas as pl
from jax.experimental.pallas import tpu as pltpu
from jax.sharding import PartitionSpec as P

HEAD_DIM = 128
ROPE_THETA = 500000.0
NORM_EPS = 1e-6
SCALE = HEAD_DIM ** -0.5
LOG2E = 1.4426950408889634
MESH = pl.DeviceIdType.MESH
BF = jnp.bfloat16
F32 = jnp.float32
CORES = 2
NT = 1024
RG = 8
MAX_HG = 4
SLOTS = 16
PER_WORD = 6
SENDS = [
    [1, 7, 2, 6, 3, 5, 4],
    [1, 7, 2, 6, 3, 5, 4],
    [1, 7, 2, 6, 3, 5, 4],
    [1, 7, 2, 6, 3, 5, 4],
    [1, 7, 2, 6, 3, 5, 4],
    [1, 7, 2, 6, 3, 5, 4],
    [1, 7, 2, 6, 3, 5, 4],
    [1, 7, 2, 6, 3, 5, 4],
]
STEPS = [
    [0, 1, 9, 2, 7, 10, 3, 8, 5, 6, 4, 13, 15, 11, 12, 14],
    [0, 1, 2, 7, 3, 15, 9, 4, 12, 6, 5, 13, 14, 10, 8, 11],
    [0, 2, 7, 1, 6, 3, 11, 5, 4, 13, 9, 14, 10, 8, 15, 12],
    [0, 1, 7, 6, 5, 2, 3, 14, 13, 11, 4, 9, 15, 10, 12, 8],
    [0, 7, 5, 2, 4, 1, 6, 9, 15, 14, 3, 12, 11, 8, 13, 10],
    [0, 7, 2, 6, 3, 5, 1, 11, 4, 14, 12, 10, 9, 8, 15, 13],
    [0, 7, 6, 1, 4, 2, 10, 3, 5, 12, 13, 9, 8, 11, 15, 14],
    [0, 1, 3, 2, 6, 5, 4, 12, 13, 11, 9, 7, 10, 14, 8, 15],
]


def lane_fold(vals):
    total = vals[:, :HEAD_DIM]
    for start in range(HEAD_DIM, vals.shape[1], HEAD_DIM):
        total = total + vals[:, start:start + HEAD_DIM]
    return total


def block_kernel(n_z, x_ref, pos_ref, wq_ref, wk_ref, wv_ref, wo_ref, freq_ref, gq_ref, gk_ref, ga_ref, y_ref,
                 wbuf, xbuf, pbuf, qbuf, kbuf, vbuf, raw, sscr, gains, tabs,
                 wsem, xsend, xrecv, psend, precv, ksend, krecv, vsend, vrecv, ysend, yrecv):
    seq_loc, width = xbuf.shape[1], xbuf.shape[2]
    heads = width // HEAD_DIM
    me = lax.axis_index('sp')
    dp = lax.axis_index('dp')
    z = me // CORES
    c = me % CORES
    other = z * CORES + (1 - c)

    def peer(zz):
        return (dp, zz * CORES + c)

    def code_at(rows, i):
        val = jnp.int32(0)
        for start in range(0, len(rows[0]), PER_WORD):
            words = [sum(v << (4 * j) for j, v in enumerate(row[start:start + PER_WORD])) for row in rows]
            word = jnp.int32(words[0])
            for q, w in enumerate(words[1:], 1):
                word = jnp.where(z == q, w, word)
            val = jnp.where(i >= start, word, val)
        return lax.shift_right_logical(val, jnp.int32(4 * (i % PER_WORD))) % 16

    def w_copy(i, ref):
        return pltpu.make_async_copy(ref, wbuf.at[i], wsem.at[i])

    w_copies = [w_copy(0, wk_ref), w_copy(1, wv_ref), w_copy(2, wq_ref), w_copy(3, wo_ref)]

    def x_copy(zz, slot):
        return pltpu.make_async_remote_copy(src_ref=x_ref.at[zz], dst_ref=xbuf.at[slot], send_sem=xsend.at[zz],
                                            recv_sem=xrecv.at[slot], device_id=peer(zz), device_id_type=MESH)

    def p_copy(zz, slot):
        return pltpu.make_async_remote_copy(src_ref=pos_ref.at[zz], dst_ref=pbuf.at[slot], send_sem=psend.at[zz],
                                            recv_sem=precv.at[slot], device_id=peer(zz), device_id_type=MESH)

    def kv_copy(buf, ssem, rsem, zz, core):
        return pltpu.make_async_remote_copy(src_ref=buf.at[zz, core], dst_ref=buf.at[zz, core], send_sem=ssem.at[zz],
                                            recv_sem=rsem.at[zz], device_id=(dp, other), device_id_type=MESH)

    def y_copy(zz, slot):
        return pltpu.make_async_remote_copy(src_ref=xbuf.at[zz], dst_ref=y_ref.at[slot], send_sem=ysend.at[zz],
                                            recv_sem=yrecv.at[slot], device_id=peer(zz), device_id_type=MESH)

    own_x = pltpu.make_async_copy(x_ref.at[z], xbuf.at[z], xrecv.at[z])
    own_p = pltpu.make_async_copy(pos_ref.at[z], pbuf.at[z], precv.at[z])
    own_x.start()
    own_p.start()
    for cp in w_copies:
        cp.start()

    for i, ref in enumerate((gq_ref, gk_ref, ga_ref)):
        for h in range(heads):
            gains[i, h] = ref[h * HEAD_DIM:(h + 1) * HEAD_DIM].astype(F32)[None, :]

    barrier = pltpu.get_barrier_semaphore()
    for d in range(1, n_z):
        pl.semaphore_signal(barrier, inc=1, device_id=peer((z + d) % n_z), device_id_type=MESH)
    pl.semaphore_signal(barrier, inc=1, device_id=(dp, other), device_id_type=MESH)
    pl.semaphore_wait(barrier, n_z)

    for i in range(n_z - 1):
        zz = (z + code_at(SENDS, i)) % n_z
        p_copy(zz, z).start()
        x_copy(zz, z).start()

    def matmul_stats(load, wi):
        per = NT // HEAD_DIM

        def tile(n, ss):
            cols = pl.ds(pl.multiple_of(n * NT, NT), NT)
            prod = jnp.dot(load(), wbuf[wi, :, cols], preferred_element_type=F32).astype(BF)
            for i in range(per):
                part = prod[:, i * HEAD_DIM:(i + 1) * HEAD_DIM]
                raw[n * per + i] = part
                wide = part.astype(F32)
                ss = ss + wide * wide
            return ss
        ss = lax.fori_loop(0, width // NT, tile, jnp.zeros((seq_loc, HEAD_DIM), F32))
        return lax.rsqrt(jnp.sum(ss, axis=-1, keepdims=True) * (1.0 / width) + NORM_EPS)

    def norm_rope(scale, gain_ref, dst):
        def some(hg, carry):
            for i in range(RG):
                h = hg * RG + i
                u = raw[h].astype(F32) * scale * gain_ref[h]
                dst[h] = (u * tabs[0] + pltpu.roll(u, HEAD_DIM // 2, 1) * tabs[1]).astype(BF)
            return carry
        lax.fori_loop(0, heads // RG, some, 0)

    def make_tables(zz):
        row = jnp.broadcast_to(pbuf[zz].astype(F32), (seq_loc, seq_loc))
        angle = jnp.transpose(row) * freq_ref[...]
        lane = lax.broadcasted_iota(jnp.int32, (seq_loc, HEAD_DIM), 1)
        sin_t = jnp.sin(angle)
        tabs[0] = jnp.cos(angle)
        tabs[1] = jnp.where(lane < HEAD_DIM // 2, -sin_t, sin_t)

    def qkv_block(zz):
        make_tables(zz)
        src = xbuf.at[zz]
        norm_rope(matmul_stats(lambda: src[...], 0), gains.at[1], kbuf.at[zz, c])

        def v_tile(n, carry):
            cols = pl.ds(pl.multiple_of(n * NT, NT), NT)
            prod = jnp.dot(src[...], wbuf[1, :, cols], preferred_element_type=F32).astype(BF)
            for i in range(NT // HEAD_DIM):
                vbuf[zz, c, n * (NT // HEAD_DIM) + i] = prod[:, i * HEAD_DIM:(i + 1) * HEAD_DIM]
            return carry
        lax.fori_loop(0, width // NT, v_tile, 0)
        kv_copy(kbuf, ksend, krecv, zz, c).start()
        q_scale = matmul_stats(lambda: src[...], 2)
        kv_copy(vbuf, vsend, vrecv, zz, c).start()
        norm_rope(q_scale, gains.at[0], qbuf.at[zz])

    own_x.wait()
    own_p.wait()
    for cp in w_copies:
        cp.wait()


    keys = CORES * seq_loc
    lim = SCALE * LOG2E

    def attend_len(zz, nk):
        hg = MAX_HG if nk * MAX_HG <= SLOTS else 2
        row = lax.broadcasted_iota(jnp.int32, (seq_loc, keys), 0) + c * seq_loc
        col = lax.broadcasted_iota(jnp.int32, (seq_loc, keys), 1)
        seen = col <= row

        def group(g, carry):
            peak = []
            for i in range(hg):
                h = g * hg + i
                q = qbuf[zz, h]
                top = None
                for kz in range(nk):
                    k = kbuf[kz, :, h].reshape(keys, HEAD_DIM)
                    s = lax.dot_general(q, k, (((1,), (1,)), ((), ())), preferred_element_type=F32)
                    if kz == nk - 1:
                        s = jnp.where(seen, s, -1e30)
                    sscr[i * nk + kz] = s
                    fold = jnp.maximum(s[:, :seq_loc], s[:, seq_loc:])
                    top = fold if top is None else jnp.maximum(top, fold)
                peak.append(jnp.max(top, axis=-1, keepdims=True))
            for i in range(hg):
                h = g * hg + i
                total = None
                probs = []
                for kz in range(nk):
                    p = jnp.exp2((sscr[i * nk + kz] - peak[i]) * lim)
                    fold = p[:, :seq_loc] + p[:, seq_loc:]
                    total = fold if total is None else total + fold
                    probs.append(p.astype(BF))
                v = jnp.concatenate([vbuf[kz, :, h].reshape(keys, HEAD_DIM) for kz in range(nk)], axis=0)
                out = jnp.dot(jnp.concatenate(probs, axis=1), v, preferred_element_type=F32)
                denom = jnp.sum(total, axis=-1, keepdims=True)
                qbuf[zz, h] = (out / denom).astype(BF)
            return carry
        lax.fori_loop(0, heads // hg, group, 0)

    def attend(zz):
        for nk in range(1, n_z + 1):
            pl.when(zz == nk - 1)(functools.partial(attend_len, zz, nk))

    def out_block(zz):
        scale = matmul_stats(lambda: jnp.concatenate([qbuf[zz, h] for h in range(heads)], axis=1), 3)

        def some(hg, carry):
            for i in range(RG):
                h = hg * RG + i
                cols = pl.ds(pl.multiple_of(h * HEAD_DIM, HEAD_DIM), HEAD_DIM)
                y = xbuf[zz, :, cols].astype(F32) + raw[h].astype(F32) * scale * gains[2, h]
                xbuf[zz, :, cols] = y.astype(BF)
            return carry
        lax.fori_loop(0, heads // RG, some, 0)

    own_y = pltpu.make_async_copy(xbuf.at[z], y_ref.at[z], yrecv.at[z])

    def step(i, done):
        code = code_at(STEPS, i)
        zz = (z + code) % n_z

        @pl.when(code < n_z)
        def _():
            @pl.when(code > 0)
            def _():
                p_copy(z, zz).wait_recv()
                x_copy(z, zz).wait_recv()
            qkv_block(zz)

        @pl.when(code >= n_z)
        def _():
            def kv_wait(j, carry):
                prev = code_at(STEPS, j)

                @pl.when(prev < n_z)
                def _():
                    src = (z + prev) % n_z
                    kv_copy(kbuf, ksend, krecv, src, 1 - c).wait_recv()
                    kv_copy(vbuf, vsend, vrecv, src, 1 - c).wait_recv()
                return carry
            lax.fori_loop(done, i, kv_wait, 0)
            attend(zz)
            out_block(zz)

            @pl.when(code > n_z)
            def _():
                y_copy(zz, z).start()

            @pl.when(code == n_z)
            def _():
                own_y.start()
        return jnp.where(code < n_z, done, i)
    lax.fori_loop(0, 2 * n_z, step, 0)

    def drain(t, carry):
        zz = (z + t) % n_z
        p_copy(zz, z).wait_send()
        x_copy(zz, z).wait_send()
        y_copy(zz, z).wait_send()
        y_copy(z, zz).wait_recv()
        return carry
    lax.fori_loop(1, n_z, drain, 0)

    def kv_drain(zz, carry):
        kv_copy(kbuf, ksend, krecv, zz, c).wait_send()
        kv_copy(vbuf, vsend, vrecv, zz, c).wait_send()
        return carry
    lax.fori_loop(0, n_z, kv_drain, 0)
    own_y.wait()


def copy_kernel(src_ref, dst_ref, buf, in_sem, out_sem):
    parts = src_ref.shape[0]
    reads = [pltpu.make_async_copy(src_ref.at[i], buf.at[i], in_sem.at[i]) for i in range(parts)]
    writes = [pltpu.make_async_copy(buf.at[i], dst_ref.at[i], out_sem.at[i]) for i in range(parts)]
    for cp in reads:
        cp.start()
    for rd, wr in zip(reads, writes):
        rd.wait()
        wr.start()
    for cp in writes:
        cp.wait()


def solution(mesh):
    n_z = mesh.shape['sp'] // CORES

    def local_block(x_loc, pos_loc, w_query, w_key, w_value, w_out, gain_q, gain_k, gain_out):
        batch, seq_loc, width = x_loc.shape
        inv_freq = 1.0 / (ROPE_THETA ** (np.arange(0, HEAD_DIM, 2, dtype=np.float32) / HEAD_DIM))
        freq = jnp.asarray(np.concatenate([inv_freq, inv_freq]).astype(np.float32)[None, :])
        heads = width // HEAD_DIM
        any_spec = pl.BlockSpec(memory_space=pl.ANY)
        vmem = pl.BlockSpec(memory_space=pltpu.VMEM)
        dma = pltpu.SemaphoreType.DMA
        y_home = pl.pallas_call(
            functools.partial(block_kernel, n_z),
            out_shape=jax.ShapeDtypeStruct(x_loc.shape, BF),
            in_specs=[any_spec] * 6 + [vmem] * 4,
            out_specs=any_spec,
            scratch_shapes=[
                pltpu.VMEM((4, width, width), BF),
                pltpu.VMEM((n_z, seq_loc, width), BF),
                pltpu.VMEM((n_z, 1, seq_loc), jnp.int32),
                pltpu.VMEM((n_z, heads, seq_loc, HEAD_DIM), BF),
                pltpu.VMEM((n_z, CORES, heads, seq_loc, HEAD_DIM), BF),
                pltpu.VMEM((n_z, CORES, heads, seq_loc, HEAD_DIM), BF),
                pltpu.VMEM((heads, seq_loc, HEAD_DIM), BF),
                pltpu.VMEM((SLOTS, seq_loc, CORES * seq_loc), F32),
                pltpu.VMEM((3, heads, 1, HEAD_DIM), F32),
                pltpu.VMEM((2, seq_loc, HEAD_DIM), F32),
                dma((4,)),
            ] + [dma((n_z,))] * 10,
            compiler_params=pltpu.CompilerParams(collective_id=0, has_side_effects=True, vmem_limit_bytes=67043328),
        )(x_loc, pos_loc[:, None, :], w_query, w_key, w_value, w_out, freq, gain_q, gain_k, gain_out)
        return pl.pallas_call(
            copy_kernel,
            out_shape=jax.ShapeDtypeStruct(x_loc.shape, BF),
            in_specs=[any_spec],
            out_specs=any_spec,
            scratch_shapes=[pltpu.VMEM(x_loc.shape, BF), dma((batch,)), dma((batch,))],
        )(y_home)

    tok_spec = P('dp', 'sp', None)
    return jax.shard_map(local_block, mesh=mesh, in_specs=(tok_spec, P('dp', 'sp'), P(), P(), P(), P(), P(), P(), P()), out_specs=tok_spec, check_vma=False)
```
